32 devices in a mesh: cells: 8 (over z, x), genes: 4 (over y, core).
Axes of the slice: x: 2, y: 2, z: 4, core: 2. Of those that a mesh axis runs over, the one named last changes fastest.
Arguments:
- expression: bfloat16 [32768, 4096], P('cells', 'genes'), may hold values from -200 to 200
- labels: int32 [32768], P('cells'), may hold values from 0 to 199, as said below
- loadings: bfloat16 [4096, 50], P('genes'), may hold values from -0.09375 to 0.09375
Outputs:
- adjusted: bfloat16 [32768, 4096], P('cells', 'genes')
- scores: float32 [32768, 50], P('cells')
The draws below stay inside these ranges and needn't reach their ends.
Inputs may be any that keep to these rules, and one draw needn't show every extreme that they name: `labels`: every batch has two or more cells.
All inputs are finite; a program needn't handle non-finite values.
Results may differ from the reference program's by a relative error of at most 0.0029.
Values sent between devices are 32-bit elements; how exact they have to be, the bound alone decides.
No kernel may reach another device: no remote copies, remote signals or barrier semaphores. Data moves between devices by JAX's collectives and lax.ppermute only.
A program may use at most 64 MiB of HBM per device.

```python
import math
import jax
import jax.numpy as jnp
from jax import lax

GENES = 4096
BATCHES = 200
COMPONENTS = 50
SWEEPS = 10
CELLS = 32768


def label_table(key):
    rare_count = BATCHES // 3
    common_count = BATCHES - rare_count
    rare_top = max(2, min(30, CELLS // (2 * BATCHES)))
    keys = jax.random.split(jax.random.fold_in(key, 11), 5)
    order = jax.random.permutation(keys[0], BATCHES).astype(jnp.int32)
    rare_ids = order[:rare_count]
    common_ids = order[rare_count:]
    rare_sizes = jax.random.randint(keys[1], (rare_count,), 2, rare_top + 1, dtype=jnp.int32)
    rare_ends = jnp.cumsum(rare_sizes).astype(jnp.int32)
    rare_total = rare_ends[rare_count - 1]
    position = jnp.arange(CELLS, dtype=jnp.int32)
    rare_slot = jnp.minimum(jnp.searchsorted(rare_ends, position, side='right').astype(jnp.int32), rare_count - 1)
    base_slot = jnp.clip((position - rare_total) // 2, 0, common_count - 1).astype(jnp.int32)
    pick_first = jax.random.randint(keys[2], (CELLS,), 0, common_count, dtype=jnp.int32)
    pick_second = jax.random.randint(keys[3], (CELLS,), 0, common_count, dtype=jnp.int32)
    extra_slot = jnp.minimum(pick_first, pick_second)
    ordered = jnp.where(position < rare_total, rare_ids[rare_slot], jnp.where(position < rare_total + 2 * common_count, common_ids[base_slot], common_ids[extra_slot]))
    shuffle = jax.random.permutation(keys[4], CELLS).astype(jnp.int32)
    return ordered[shuffle].astype(jnp.int32)


def draw_labels(key, part):
    return label_table(key)


def draw_expression(key, part):
    labels = label_table(key)
    keys = jax.random.split(jax.random.fold_in(key, 23), 6)
    gene_scale = jnp.exp(jax.random.uniform(keys[0], (GENES,), jnp.float32, 0.0, jnp.log(10.0)))
    noise = jnp.clip(jax.random.normal(keys[4], (CELLS, GENES), jnp.float32), -5.0, 5.0)
    ramp_low = 0.5
    ramp_high = 3.0
    width_low = 0.2
    width_high = 0.8
    position = jnp.arange(GENES, dtype=jnp.float32) / (GENES - 1.0)
    gene_ramp = ramp_low + (ramp_high - ramp_low) * position
    gene_width = width_low + (width_high - width_low) * position
    gene_mean = jax.random.uniform(keys[1], (GENES,), jnp.float32, -2.0, 2.0)
    batch_offset = jax.random.uniform(keys[5], (BATCHES,), jnp.float32, -1.0, 1.0)
    shift = 0.4 * gene_ramp[None, :] * (jnp.clip(jax.random.normal(keys[2], (BATCHES, GENES), jnp.float32), -4.0, 4.0) + batch_offset[:, None])
    batch_scale = jnp.exp(jax.random.uniform(keys[3], (BATCHES, GENES), jnp.float32, -1.0, 1.0) * gene_width[None, :])
    values = gene_mean[None, :] + gene_scale[None, :] * (shift[labels] + batch_scale[labels] * noise) / 3.0
    return values.astype(jnp.bfloat16)


def shard_levels(rng, shape, pieces, least, largest):
    level, own = 1.0, jax.random.fold_in(rng, 6)
    for dim, shards_of in pieces:
        steps = jnp.exp(jax.random.uniform(jax.random.fold_in(own, dim), (shards_of,), jnp.float32, least / len(pieces), largest / len(pieces)))
        level = level * jnp.repeat(steps, shape[dim] // shards_of).reshape([-1 if axis == dim else 1 for axis in range(len(shape))])
    return level


def gaussian(own_key, shape, width, limit, cuts=(), kind=jnp.bfloat16):
    loudness = shard_levels(own_key, shape, cuts, -0.22, 0.18) if cuts else 1.0
    result = jax.random.normal(own_key, shape, jnp.float32) * width * loudness
    return jnp.minimum(jnp.maximum(result, -limit), limit).astype(kind)


def setup_inputs(seed: int = 0) -> dict:
    key_of = jax.random.split(jax.random.key(seed), 4)
    expression = draw_expression(jax.random.fold_in(key_of[3], 71), 0)
    labels = draw_labels(jax.random.fold_in(key_of[3], 71), 0)
    loadings = gaussian(key_of[2], (GENES, COMPONENTS), GENES ** -0.5, 0.09375, ((0, 4),))
    return {"expression": expression, "labels": labels, "loadings": loadings}


def batch_moments(sum_one, sum_two, counts, total_cells):
    grand = lax.optimization_barrier(jnp.sum(sum_one, axis=0)) / total_cells
    within = sum_two - sum_one * sum_one / counts[:, None]
    pooled = lax.optimization_barrier(jnp.sum(within, axis=0)) / total_cells + 1e-06
    gene_sd = jnp.sqrt(pooled)
    gamma_hat = (sum_one / counts[:, None] - grand[None, :]) / gene_sd[None, :]
    delta_hat = within / ((counts[:, None] - 1.0) * pooled[None, :])
    return (grand, gene_sd, gamma_hat, delta_hat)

def shrink(gamma_hat, delta_hat, counts):
    gamma_bar = lax.optimization_barrier(jnp.sum(gamma_hat, axis=1)) / GENES
    tau_sq = (lax.optimization_barrier(jnp.sum(gamma_hat * gamma_hat, axis=1)) - GENES * gamma_bar * gamma_bar) / (GENES - 1)
    delta_mean = lax.optimization_barrier(jnp.sum(delta_hat, axis=1)) / GENES
    delta_var = (lax.optimization_barrier(jnp.sum(delta_hat * delta_hat, axis=1)) - GENES * delta_mean * delta_mean) / (GENES - 1) + 1e-06
    a_prior = (2.0 * delta_var + delta_mean * delta_mean) / delta_var
    b_prior = (delta_mean * delta_var + delta_mean ** 3) / delta_var
    weight = counts[:, None]

    def sweep(sweep_index, state):
        gamma_now, delta_now = state
        gamma_next = (weight * tau_sq[:, None] * gamma_hat + delta_now * gamma_bar[:, None]) / (weight * tau_sq[:, None] + delta_now)
        sum_sq = (weight - 1.0) * delta_hat + weight * (gamma_hat - gamma_next) ** 2
        delta_next = (0.5 * sum_sq + b_prior[:, None]) / (0.5 * weight + a_prior[:, None] - 1.0)
        return (gamma_next, delta_next)
    gamma_star, delta_star = lax.fori_loop(0, SWEEPS, sweep, (gamma_hat, delta_hat))
    return (gamma_star, 1.0 / jnp.sqrt(delta_star))

def reference(expression, labels, loadings):
    block_rows = math.gcd(CELLS, 4096)
    block_count = CELLS // block_rows
    indices = jnp.arange(block_count, dtype=jnp.int32)

    def accumulate(totals, block_index):
        start = block_index * block_rows
        values = lax.dynamic_slice_in_dim(expression, start, block_rows, 0).astype(jnp.float32)
        local_labels = lax.dynamic_slice_in_dim(labels, start, block_rows, 0)
        first = jax.ops.segment_sum(values, local_labels, BATCHES)
        second = jax.ops.segment_sum(values * values, local_labels, BATCHES)
        number = jax.ops.segment_sum(jnp.ones((block_rows,), jnp.float32), local_labels, BATCHES)
        return ((totals[0] + first, totals[1] + second, totals[2] + number), None)
    zeros_table = jnp.zeros((BATCHES, GENES), jnp.float32)
    (sum_one, sum_two, counts), unused = lax.scan(accumulate, (zeros_table, zeros_table, jnp.zeros((BATCHES,), jnp.float32)), indices)
    grand, gene_sd, gamma_hat, delta_hat = batch_moments(sum_one, sum_two, counts, CELLS)
    gamma_star, scale_star = shrink(gamma_hat, delta_hat, counts)

    def adjust(block_index):
        start = block_index * block_rows
        values = lax.dynamic_slice_in_dim(expression, start, block_rows, 0).astype(jnp.float32)
        local_labels = lax.dynamic_slice_in_dim(labels, start, block_rows, 0)
        shifted = (values - grand[None, :]) / gene_sd[None, :]
        standard = (shifted - gamma_star[local_labels]) * scale_star[local_labels]
        adjusted = (gene_sd[None, :] * standard + grand[None, :]).astype(jnp.bfloat16)
        standard_low = standard.astype(jnp.bfloat16)
        partial_value = jnp.dot(standard_low, loadings, preferred_element_type=jnp.float32)
        return (adjusted, partial_value)
    adjusted, scores = lax.map(adjust, indices)
    return (adjusted.reshape(CELLS, GENES), scores.reshape(CELLS, COMPONENTS))
```

```python
import functools
import math

import jax
import jax.numpy as jnp
from jax import lax
from jax.experimental import pallas as pl
from jax.experimental.pallas import tpu as pltpu
from jax.sharding import PartitionSpec as P

BATCHES = 200
SWEEPS = 10
PADDED = 256
ROW_TILE = 512
GENE_TILE = 256


def iota(shape, axis):
    return lax.broadcasted_iota(jnp.int32, shape, axis)


def to_row(column, row, width):
    shape = (BATCHES, width)
    hit = iota(shape, 0) == iota(shape, 1) + row * width
    return jnp.sum(jnp.where(hit, column, 0.0), axis=0, keepdims=True)


def to_column(rows, width):
    shape = (BATCHES, width)
    total = jnp.zeros(shape, jnp.float32)
    for row, values in enumerate(rows):
        hit = iota(shape, 0) == iota(shape, 1) + row * width
        total = total + jnp.where(hit, values, 0.0)
    return jnp.sum(total, axis=1, keepdims=True)


def count_rows(width):
    return -(-BATCHES // width)


def packed_rows(width):
    return 2 * BATCHES + 8 * (-(-count_rows(width) // 8))


def moments_kernel(x_ref, labels_ref, out_ref, one_ref, two_ref, count_ref, *, width):
    step = pl.program_id(0)
    values = x_ref[...]
    rows = values.shape[0]
    hit = iota((PADDED, rows), 0) == labels_ref[0]
    members = jnp.where(hit, 1.0, 0.0)
    number = jnp.sum(members, axis=1, keepdims=True)
    members = members.astype(jnp.bfloat16)
    wide = values.astype(jnp.float32)
    square = wide * wide
    upper = square.astype(jnp.bfloat16)
    lower = (square - upper.astype(jnp.float32)).astype(jnp.bfloat16)
    first = jnp.dot(members, values, preferred_element_type=jnp.float32)
    second = jnp.dot(
        jnp.concatenate([members, members], axis=1),
        jnp.concatenate([upper, lower], axis=0),
        preferred_element_type=jnp.float32,
    )

    @pl.when(step == 0)
    def _():
        one_ref[...] = first
        two_ref[...] = second
        count_ref[...] = jnp.broadcast_to(number, count_ref.shape)

    @pl.when(step > 0)
    def _():
        one_ref[...] += first
        two_ref[...] += second
        count_ref[...] += jnp.broadcast_to(number, count_ref.shape)

    @pl.when(step == pl.num_programs(0) - 1)
    def _():
        column = count_ref[0:BATCHES, 0:1]
        counts = [to_row(column, row, width) for row in range(count_rows(width))]
        spare = packed_rows(width) - 2 * BATCHES
        for shard in range(out_ref.shape[0]):
            cols = slice(shard * width, (shard + 1) * width)
            out_ref[shard, 0:BATCHES, :] = one_ref[0:BATCHES, cols]
            out_ref[shard, BATCHES : 2 * BATCHES, :] = two_ref[0:BATCHES, cols]
            out_ref[shard, 2 * BATCHES :, :] = jnp.zeros((spare, width), jnp.float32)
            for row, line in enumerate(counts):
                out_ref[shard, 2 * BATCHES + row : 2 * BATCHES + row + 1, :] = line


def batch_moments(sums_ref, width, total_cells):
    sum_one = sums_ref[0:BATCHES, :]
    sum_two = sums_ref[BATCHES : 2 * BATCHES, :]
    lines = [
        sums_ref[2 * BATCHES + row : 2 * BATCHES + row + 1, :] for row in range(count_rows(width))
    ]
    counts = to_column(lines, width)
    grand = jnp.sum(sum_one, axis=0, keepdims=True) / total_cells
    within = sum_two - sum_one * sum_one / counts
    pooled = jnp.sum(within, axis=0, keepdims=True) / total_cells + 1e-06
    gene_sd = jnp.sqrt(pooled)
    gamma_hat = (sum_one / counts - grand) / gene_sd
    delta_hat = within / ((counts - 1.0) * pooled)
    return counts, grand, gene_sd, gamma_hat, delta_hat


def terms_kernel(sums_ref, terms_ref, *, width, total_cells):
    _, _, _, gamma_hat, delta_hat = batch_moments(sums_ref, width, total_cells)
    for row, values in enumerate((gamma_hat, gamma_hat * gamma_hat, delta_hat, delta_hat * delta_hat)):
        column = jnp.sum(values, axis=1, keepdims=True)
        terms_ref[row : row + 1, :] = to_row(column, 0, PADDED)


def shrink_kernel(sums_ref, terms_ref, out_ref, *, width, total_cells, genes):
    counts, grand, gene_sd, gamma_hat, delta_hat = batch_moments(sums_ref, width, total_cells)
    sum_gamma, sum_gamma_sq, sum_delta, sum_delta_sq = (
        to_column([terms_ref[row : row + 1, :]], PADDED) for row in range(4)
    )
    gamma_bar = sum_gamma / genes
    tau_sq = (sum_gamma_sq - genes * gamma_bar * gamma_bar) / (genes - 1)
    delta_mean = sum_delta / genes
    delta_var = (sum_delta_sq - genes * delta_mean * delta_mean) / (genes - 1) + 1e-06
    a_prior = (2.0 * delta_var + delta_mean * delta_mean) / delta_var
    b_prior = (delta_mean * delta_var + delta_mean * delta_mean * delta_mean) / delta_var
    pull = counts * tau_sq
    pulled = pull * gamma_hat
    spread = (counts - 1.0) * delta_hat
    bottom = 0.5 * counts + a_prior - 1.0

    def sweep(_, state):
        _, delta_now = state
        gamma_next = (pulled + delta_now * gamma_bar) / (pull + delta_now)
        off = gamma_hat - gamma_next
        sum_sq = spread + counts * (off * off)
        return gamma_next, (0.5 * sum_sq + b_prior) / bottom

    gamma_star, delta_star = lax.fori_loop(0, SWEEPS, sweep, (gamma_hat, delta_hat))
    out_ref[0:BATCHES, :] = gamma_star
    out_ref[BATCHES : 2 * BATCHES, :] = 1.0 / jnp.sqrt(delta_star)
    out_ref[2 * BATCHES :, :] = jnp.zeros((out_ref.shape[0] - 2 * BATCHES, width), jnp.float32)
    out_ref[2 * BATCHES : 2 * BATCHES + 1, :] = grand
    out_ref[2 * BATCHES + 1 : 2 * BATCHES + 2, :] = gene_sd


def adjust_kernel(
    order_ref, x_ref, labels_ref, table_ref, loadings_ref, adjusted_ref, scores_ref,
    gamma_ref, scale_ref, gene_ref, weight_ref, members_ref, *, width
):
    rows, cols = x_ref.shape
    components = loadings_ref.shape[0]

    @pl.when(pl.program_id(0) == 0)
    def _():
        weight_ref[...] = jnp.zeros(weight_ref.shape, weight_ref.dtype)
        weight_ref[0:components, :] = loadings_ref[...]
        blank = jnp.zeros((PADDED - BATCHES, width), jnp.float32)
        shards = table_ref.shape[0]
        for place in range(shards):
            span = slice(place * width, (place + 1) * width)
            shard = order_ref[place]
            for part, target in ((0, gamma_ref), (1, scale_ref)):
                table = jnp.concatenate(
                    [table_ref[shard, part * BATCHES : (part + 1) * BATCHES, :], blank], axis=0
                )
                upper = table.astype(jnp.bfloat16)
                target[0:PADDED, span] = upper
                target[PADDED:, span] = (table - upper.astype(jnp.float32)).astype(jnp.bfloat16)
            grand = table_ref[shard, 2 * BATCHES : 2 * BATCHES + 1, :]
            gene_sd = table_ref[shard, 2 * BATCHES + 1 : 2 * BATCHES + 2, :]
            gene_ref[0:1, span] = grand
            gene_ref[1:2, span] = gene_sd
            gene_ref[2:3, span] = 1.0 / gene_sd

    lane = iota((128, PADDED), 1)
    for chunk in range(rows // 128):
        line = jnp.broadcast_to(labels_ref[0, chunk : chunk + 1, :], (128, 128))
        down = jnp.transpose(line)
        hit = lane == jnp.concatenate([down] * (PADDED // 128), axis=1)
        members = jnp.where(hit, 1.0, 0.0).astype(jnp.bfloat16)
        members_ref[chunk * 128 : (chunk + 1) * 128, 0:PADDED] = members
        members_ref[chunk * 128 : (chunk + 1) * 128, PADDED:] = members

    members = members_ref[...]
    tile = math.gcd(cols, GENE_TILE)
    scores = jnp.zeros((rows, weight_ref.shape[0]), jnp.float32)
    for start in range(0, cols, tile):
        span = slice(start, start + tile)
        gamma = jnp.dot(members, gamma_ref[:, span], preferred_element_type=jnp.float32)
        scale = jnp.dot(members, scale_ref[:, span], preferred_element_type=jnp.float32)
        grand = gene_ref[0:1, span]
        gene_sd = gene_ref[1:2, span]
        shifted = (x_ref[:, span].astype(jnp.float32) - grand) * gene_ref[2:3, span]
        standard = (shifted - gamma) * scale
        adjusted_ref[:, span] = (gene_sd * standard + grand).astype(jnp.bfloat16)
        scores = scores + lax.dot_general(
            standard.astype(jnp.bfloat16),
            weight_ref[:, span],
            (((1,), (1,)), ((), ())),
            preferred_element_type=jnp.float32,
        )
    scores_ref[...] = jnp.transpose(scores)[0:components, :]


def exchange(value, axis, offset):
    size = lax.axis_size(axis)
    return lax.ppermute(value, axis, [(source, source ^ offset) for source in range(size)])


def scatter_sum(table):
    place = lax.axis_index("cells")
    total = lax.dynamic_index_in_dim(table, place, 0, False)
    for offset in range(1, lax.axis_size("cells")):
        block = lax.dynamic_index_in_dim(table, place ^ offset, 0, False)
        total = total + exchange(block, "cells", offset)
    return total


def gather(table):
    size = lax.axis_size("cells")
    blocks = [table]
    for offset in range(1, size):
        blocks.append(lax.ppermute(table, "cells", [(s, (s + offset) % size) for s in range(size)]))
    place = lax.axis_index("cells")
    order = (place - jnp.arange(size, dtype=jnp.int32)) % size
    return jnp.stack(blocks), order.astype(jnp.int32)


def small_sum(value):
    for axis in ("cells", "genes"):
        parts = [exchange(value, axis, offset) for offset in range(1, lax.axis_size(axis))]
        for part in parts:
            value = value + part
    return value


def sum_over_genes(scores):
    components, rows = scores.shape
    size = lax.axis_size("genes")
    low = lax.axis_index("genes") % 2
    halves = scores.reshape(2, components // 2, rows)
    kept = lax.dynamic_index_in_dim(halves, low, 0, False)
    total = kept + exchange(lax.dynamic_index_in_dim(halves, 1 - low, 0, False), "genes", 1)
    offset = 2
    while offset < size:
        total = total + exchange(total, "genes", offset)
        offset *= 2
    other = exchange(total, "genes", 1)
    first = jnp.where(low == 0, total, other)
    second = jnp.where(low == 0, other, total)
    return jnp.concatenate([first, second], axis=0)


def body(expression, labels, loadings):
    rows, cols = expression.shape
    cell_shards = lax.axis_size("cells")
    width = cols // cell_shards
    total_cells = rows * cell_shards
    genes = cols * lax.axis_size("genes")
    components = loadings.shape[1]
    packed = packed_rows(width)
    tile = math.gcd(rows, ROW_TILE)
    steps = rows // tile
    f32 = jnp.float32

    sums = pl.pallas_call(
        functools.partial(moments_kernel, width=width),
        grid=(steps,),
        in_specs=[
            pl.BlockSpec((tile, cols), lambda i: (i, 0)),
            pl.BlockSpec((1, 1, tile), lambda i: (i, 0, 0)),
        ],
        out_specs=pl.BlockSpec((cell_shards, packed, width), lambda i: (0, 0, 0)),
        out_shape=jax.ShapeDtypeStruct((cell_shards, packed, width), f32),
        scratch_shapes=[
            pltpu.VMEM((PADDED, cols), f32),
            pltpu.VMEM((PADDED, cols), f32),
            pltpu.VMEM((PADDED, 128), f32),
        ],
        name="moments",
    )(expression, labels.reshape(steps, 1, tile))
    sums = scatter_sum(sums)

    terms = pl.pallas_call(
        functools.partial(terms_kernel, width=width, total_cells=total_cells),
        out_shape=jax.ShapeDtypeStruct((4, PADDED), f32),
        name="terms",
    )(sums)
    terms = small_sum(terms)
    table = pl.pallas_call(
        functools.partial(shrink_kernel, width=width, total_cells=total_cells, genes=genes),
        out_shape=jax.ShapeDtypeStruct((packed, width), f32),
        name="shrink",
    )(sums, terms)
    table, order = gather(table)

    adjusted, scores = pl.pallas_call(
        functools.partial(adjust_kernel, width=width),
        grid=(steps,),
        in_specs=[
            pl.BlockSpec(memory_space=pltpu.SMEM),
            pl.BlockSpec((tile, cols), lambda i: (i, 0)),
            pl.BlockSpec((1, tile // 128, 128), lambda i: (i, 0, 0)),
            pl.BlockSpec((cell_shards, packed, width), lambda i: (0, 0, 0)),
            pl.BlockSpec((components, cols), lambda i: (0, 0)),
        ],
        out_specs=[
            pl.BlockSpec((tile, cols), lambda i: (i, 0)),
            pl.BlockSpec((components, tile), lambda i: (0, i)),
        ],
        out_shape=[
            jax.ShapeDtypeStruct((rows, cols), jnp.bfloat16),
            jax.ShapeDtypeStruct((components, rows), f32),
        ],
        scratch_shapes=[
            pltpu.VMEM((2 * PADDED, cols), jnp.bfloat16),
            pltpu.VMEM((2 * PADDED, cols), jnp.bfloat16),
            pltpu.VMEM((8, cols), f32),
            pltpu.VMEM((128, cols), jnp.bfloat16),
            pltpu.VMEM((tile, 2 * PADDED), jnp.bfloat16),
        ],
        name="adjust",
    )(order, expression, labels.reshape(steps, tile // 128, 128), table, loadings.T)
    return adjusted, sum_over_genes(scores).T


def solution(mesh):
    placed = (P("cells", "genes"), P("cells"), P("genes", None))
    return jax.shard_map(
        body,
        mesh=mesh,
        in_specs=placed,
        out_specs=(P("cells", "genes"), P("cells", None)),
        check_vma=False,
    )
```

```python
import functools
import math

import jax
import jax.numpy as jnp
from jax import lax
from jax.experimental import pallas as pl
from jax.experimental.pallas import tpu as pltpu
from jax.sharding import PartitionSpec as P

BATCHES = 200
SWEEPS = 10
PADDED = 256
ROW_TILE = 512
GENE_TILE = 256


def iota(shape, axis):
    return lax.broadcasted_iota(jnp.int32, shape, axis)


def to_row(column, row, width):
    shape = (BATCHES, width)
    hit = iota(shape, 0) == iota(shape, 1) + row * width
    return jnp.sum(jnp.where(hit, column, 0.0), axis=0, keepdims=True)


def to_column(rows, width):
    shape = (BATCHES, width)
    total = jnp.zeros(shape, jnp.float32)
    for row, values in enumerate(rows):
        hit = iota(shape, 0) == iota(shape, 1) + row * width
        total = total + jnp.where(hit, values, 0.0)
    return jnp.sum(total, axis=1, keepdims=True)


def count_rows(width):
    return -(-BATCHES // width)


def packed_rows(width):
    return BATCHES + 8 * (-(-count_rows(width) // 8))


def orders(size):
    bits = [1 << bit for bit in range(size.bit_length() - 1)]
    if len(bits) < 3:
        return bits, bits[::-1]
    along = [bits[1]] + [low | high for low, high in zip(bits[1:], bits[2:])]
    return [bits[0]] + along, along + [bits[0]]


def places(masks):
    offsets = [0]
    for mask in reversed(masks):
        offsets = offsets + [offset ^ mask for offset in offsets]
    return offsets


def moments_kernel(order_ref, x_ref, labels_ref, first_ref, second_ref, one_ref, two_ref, count_ref, *, width):
    step = pl.program_id(0)
    values = x_ref[...]
    rows = values.shape[0]
    hit = iota((PADDED, rows), 0) == labels_ref[0]
    members = jnp.where(hit, 1.0, 0.0)
    number = jnp.sum(members, axis=1, keepdims=True)
    members = members.astype(jnp.bfloat16)
    wide = values.astype(jnp.float32)
    square = wide * wide
    upper = square.astype(jnp.bfloat16)
    lower = (square - upper.astype(jnp.float32)).astype(jnp.bfloat16)
    first = jnp.dot(members, values, preferred_element_type=jnp.float32)
    second = jnp.dot(
        jnp.concatenate([members, members], axis=1),
        jnp.concatenate([upper, lower], axis=0),
        preferred_element_type=jnp.float32,
    )

    @pl.when(step == 0)
    def _():
        one_ref[...] = first
        two_ref[...] = second
        count_ref[...] = jnp.broadcast_to(number, count_ref.shape)

    @pl.when(step > 0)
    def _():
        one_ref[...] += first
        two_ref[...] += second
        count_ref[...] += jnp.broadcast_to(number, count_ref.shape)

    @pl.when(step == pl.num_programs(0) - 1)
    def _():
        column = count_ref[0:BATCHES, 0:1]
        counts = [to_row(column, row, width) for row in range(count_rows(width))]
        spare = packed_rows(width) - BATCHES
        for shard in range(first_ref.shape[0]):
            cols = slice(shard * width, (shard + 1) * width)
            first_ref[order_ref[0, shard]] = one_ref[0:BATCHES, cols]
            place = order_ref[1, shard]
            second_ref[place, 0:BATCHES, :] = two_ref[0:BATCHES, cols]
            second_ref[place, BATCHES:, :] = jnp.zeros((spare, width), jnp.float32)
            for row, line in enumerate(counts):
                second_ref[place, BATCHES + row : BATCHES + row + 1, :] = line


def batch_moments(first_ref, second_ref, width, total_cells):
    sum_one = first_ref[...]
    sum_two = second_ref[0:BATCHES, :]
    lines = [second_ref[BATCHES + row : BATCHES + row + 1, :] for row in range(count_rows(width))]
    counts = to_column(lines, width)
    grand = jnp.sum(sum_one, axis=0, keepdims=True) / total_cells
    within = sum_two - sum_one * sum_one / counts
    pooled = jnp.sum(within, axis=0, keepdims=True) / total_cells + 1e-06
    gene_sd = jnp.sqrt(pooled)
    gamma_hat = (sum_one / counts - grand) / gene_sd
    delta_hat = within / ((counts - 1.0) * pooled)
    return counts, grand, gene_sd, gamma_hat, delta_hat


def terms_kernel(first_ref, second_ref, terms_ref, *, width, total_cells):
    _, _, _, gamma_hat, delta_hat = batch_moments(
        first_ref, second_ref, width, total_cells
    )
    for row, values in enumerate((gamma_hat, gamma_hat * gamma_hat, delta_hat, delta_hat * delta_hat)):
        column = jnp.sum(values, axis=1, keepdims=True)
        terms_ref[row : row + 1, :] = to_row(column, 0, PADDED)


def shrink_kernel(first_ref, second_ref, terms_ref, gamma_ref, scale_ref, *, width, total_cells, genes):
    counts, grand, gene_sd, gamma_hat, delta_hat = batch_moments(
        first_ref, second_ref, width, total_cells
    )
    sum_gamma, sum_gamma_sq, sum_delta, sum_delta_sq = (
        to_column([terms_ref[row : row + 1, :]], PADDED) for row in range(4)
    )
    gamma_bar = sum_gamma / genes
    tau_sq = (sum_gamma_sq - genes * gamma_bar * gamma_bar) / (genes - 1)
    delta_mean = sum_delta / genes
    delta_var = (sum_delta_sq - genes * delta_mean * delta_mean) / (genes - 1) + 1e-06
    a_prior = (2.0 * delta_var + delta_mean * delta_mean) / delta_var
    b_prior = (delta_mean * delta_var + delta_mean * delta_mean * delta_mean) / delta_var
    pull = counts * tau_sq
    pulled = pull * gamma_hat
    spread = (counts - 1.0) * delta_hat
    bottom = 0.5 * counts + a_prior - 1.0

    def sweep(_, state):
        _, delta_now = state
        gamma_next = (pulled + delta_now * gamma_bar) / (pull + delta_now)
        off = gamma_hat - gamma_next
        sum_sq = spread + counts * (off * off)
        return gamma_next, (0.5 * sum_sq + b_prior) / bottom

    gamma_star, delta_star = lax.fori_loop(0, SWEEPS, sweep, (gamma_hat, delta_hat))
    gamma_ref[...] = gamma_star
    scale_ref[0:BATCHES, :] = 1.0 / jnp.sqrt(delta_star)
    scale_ref[BATCHES:, :] = jnp.zeros((scale_ref.shape[0] - BATCHES, width), jnp.float32)
    scale_ref[BATCHES : BATCHES + 1, :] = grand
    scale_ref[BATCHES + 1 : BATCHES + 2, :] = gene_sd


def adjust_kernel(
    order_ref, x_ref, labels_ref, gamma_all_ref, scale_all_ref, loadings_ref, adjusted_ref, scores_ref,
    gamma_ref, scale_ref, gene_ref, weight_ref, members_ref, *, width
):
    rows, cols = x_ref.shape
    components = loadings_ref.shape[0]

    @pl.when(pl.program_id(0) == 0)
    def _():
        weight_ref[...] = jnp.zeros(weight_ref.shape, weight_ref.dtype)
        weight_ref[0:components, :] = loadings_ref[...]
        blank = jnp.zeros((PADDED - BATCHES, width), jnp.float32)
        for shard in range(gamma_all_ref.shape[0]):
            span = slice(shard * width, (shard + 1) * width)
            place = order_ref[1, shard]
            gamma = gamma_all_ref[order_ref[0, shard]]
            scale = scale_all_ref[place, 0:BATCHES, :]
            for rows_of, target in ((gamma, gamma_ref), (scale, scale_ref)):
                table = jnp.concatenate([rows_of, blank], axis=0)
                upper = table.astype(jnp.bfloat16)
                target[0:PADDED, span] = upper
                target[PADDED:, span] = (table - upper.astype(jnp.float32)).astype(jnp.bfloat16)
            grand = scale_all_ref[place, BATCHES : BATCHES + 1, :]
            gene_sd = scale_all_ref[place, BATCHES + 1 : BATCHES + 2, :]
            gene_ref[0:1, span] = grand
            gene_ref[1:2, span] = gene_sd
            gene_ref[2:3, span] = 1.0 / gene_sd

    lane = iota((128, PADDED), 1)
    for chunk in range(rows // 128):
        line = jnp.broadcast_to(labels_ref[0, chunk : chunk + 1, :], (128, 128))
        down = jnp.transpose(line)
        hit = lane == jnp.concatenate([down] * (PADDED // 128), axis=1)
        members = jnp.where(hit, 1.0, 0.0).astype(jnp.bfloat16)
        members_ref[chunk * 128 : (chunk + 1) * 128, 0:PADDED] = members
        members_ref[chunk * 128 : (chunk + 1) * 128, PADDED:] = members

    members = members_ref[...]
    tile = math.gcd(cols, GENE_TILE)
    scores = jnp.zeros((rows, weight_ref.shape[0]), jnp.float32)
    for start in range(0, cols, tile):
        span = slice(start, start + tile)
        gamma = jnp.dot(members, gamma_ref[:, span], preferred_element_type=jnp.float32)
        scale = jnp.dot(members, scale_ref[:, span], preferred_element_type=jnp.float32)
        grand = gene_ref[0:1, span]
        gene_sd = gene_ref[1:2, span]
        shifted = (x_ref[:, span].astype(jnp.float32) - grand) * gene_ref[2:3, span]
        standard = (shifted - gamma) * scale
        adjusted_ref[:, span] = (gene_sd * standard + grand).astype(jnp.bfloat16)
        scores = scores + lax.dot_general(
            standard.astype(jnp.bfloat16),
            weight_ref[:, span],
            (((1,), (1,)), ((), ())),
            preferred_element_type=jnp.float32,
        )
    scores_ref[...] = jnp.transpose(scores)[0:components, :]


def exchange(value, axis, offset):
    size = lax.axis_size(axis)
    return lax.ppermute(value, axis, [(source, source ^ offset) for source in range(size)])


def scatter_sum(tables, masks_of):
    tables = list(tables)
    for step in range(len(masks_of[0])):
        half = tables[0].shape[0] // 2
        taken = [
            exchange(table[half:], "cells", masks[step]) for table, masks in zip(tables, masks_of)
        ]
        tables = [table[:half] + part for table, part in zip(tables, taken)]
    return [table[0] for table in tables]


def gather(tables, masks_of):
    tables = [table[None] for table in tables]
    for step in reversed(range(len(masks_of[0]))):
        taken = [exchange(table, "cells", masks[step]) for table, masks in zip(tables, masks_of)]
        tables = [jnp.concatenate(pair, axis=0) for pair in zip(tables, taken)]
    return tables


def small_sum(value):
    for axis in ("cells", "genes"):
        parts = [exchange(value, axis, offset) for offset in range(1, lax.axis_size(axis))]
        for part in parts:
            value = value + part
    return value


def sum_over_genes(scores):
    components, rows = scores.shape
    size = lax.axis_size("genes")
    low = lax.axis_index("genes") % 2
    halves = scores.reshape(2, components // 2, rows)
    kept = lax.dynamic_index_in_dim(halves, low, 0, False)
    total = kept + exchange(lax.dynamic_index_in_dim(halves, 1 - low, 0, False), "genes", 1)
    offset = 2
    while offset < size:
        total = total + exchange(total, "genes", offset)
        offset *= 2
    other = exchange(total, "genes", 1)
    first = jnp.where(low == 0, total, other)
    second = jnp.where(low == 0, other, total)
    return jnp.concatenate([first, second], axis=0)


def body(expression, labels, loadings):
    rows, cols = expression.shape
    cell_shards = lax.axis_size("cells")
    width = cols // cell_shards
    total_cells = rows * cell_shards
    genes = cols * lax.axis_size("genes")
    components = loadings.shape[1]
    packed = packed_rows(width)
    tile = math.gcd(rows, ROW_TILE)
    steps = rows // tile
    f32 = jnp.float32

    masks_of = orders(cell_shards)
    found = []
    for masks in masks_of:
        offsets = places(masks)
        place_of = [offsets.index(offset) for offset in range(cell_shards)]
        found.append([[place_of[own ^ shard] for shard in range(cell_shards)] for own in range(cell_shards)])
    order = lax.dynamic_index_in_dim(
        jnp.asarray(list(zip(*found)), jnp.int32), lax.axis_index("cells"), 0, False
    )
    shapes = [(BATCHES, width), (packed, width)]
    blocks = [(cell_shards, *shape) for shape in shapes]
    block_specs = [pl.BlockSpec(block, lambda i: (0, 0, 0)) for block in blocks]

    sums = pl.pallas_call(
        functools.partial(moments_kernel, width=width),
        grid=(steps,),
        in_specs=[
            pl.BlockSpec(memory_space=pltpu.SMEM),
            pl.BlockSpec((tile, cols), lambda i: (i, 0)),
            pl.BlockSpec((1, 1, tile), lambda i: (i, 0, 0)),
        ],
        out_specs=block_specs,
        out_shape=[jax.ShapeDtypeStruct(block, f32) for block in blocks],
        scratch_shapes=[
            pltpu.VMEM((PADDED, cols), f32),
            pltpu.VMEM((PADDED, cols), f32),
            pltpu.VMEM((PADDED, 128), f32),
        ],
        name="moments",
    )(order, expression, labels.reshape(steps, 1, tile))
    sums = scatter_sum(sums, masks_of)

    terms = pl.pallas_call(
        functools.partial(terms_kernel, width=width, total_cells=total_cells),
        out_shape=jax.ShapeDtypeStruct((4, PADDED), f32),
        name="terms",
    )(*sums)
    terms = small_sum(terms)
    tables = pl.pallas_call(
        functools.partial(shrink_kernel, width=width, total_cells=total_cells, genes=genes),
        out_shape=[jax.ShapeDtypeStruct(shape, f32) for shape in shapes],
        name="shrink",
    )(*sums, terms)
    tables = gather(tables, masks_of)

    adjusted, scores = pl.pallas_call(
        functools.partial(adjust_kernel, width=width),
        grid=(steps,),
        in_specs=[
            pl.BlockSpec(memory_space=pltpu.SMEM),
            pl.BlockSpec((tile, cols), lambda i: (i, 0)),
            pl.BlockSpec((1, tile // 128, 128), lambda i: (i, 0, 0)),
            *block_specs,
            pl.BlockSpec((components, cols), lambda i: (0, 0)),
        ],
        out_specs=[
            pl.BlockSpec((tile, cols), lambda i: (i, 0)),
            pl.BlockSpec((components, tile), lambda i: (0, i)),
        ],
        out_shape=[
            jax.ShapeDtypeStruct((rows, cols), jnp.bfloat16),
            jax.ShapeDtypeStruct((components, rows), f32),
        ],
        scratch_shapes=[
            pltpu.VMEM((2 * PADDED, cols), jnp.bfloat16),
            pltpu.VMEM((2 * PADDED, cols), jnp.bfloat16),
            pltpu.VMEM((8, cols), f32),
            pltpu.VMEM((128, cols), jnp.bfloat16),
            pltpu.VMEM((tile, 2 * PADDED), jnp.bfloat16),
        ],
        name="adjust",
    )(order, expression, labels.reshape(steps, tile // 128, 128), *tables, loadings.T)
    return adjusted, sum_over_genes(scores).T


def solution(mesh):
    placed = (P("cells", "genes"), P("cells"), P("genes", None))
    return jax.shard_map(
        body,
        mesh=mesh,
        in_specs=placed,
        out_specs=(P("cells", "genes"), P("cells", None)),
        check_vma=False,
    )
```
